32 devices in a mesh: dp: 4 (over y, x), expert: 8 (over z, core).
Axes of the slice: x: 2, y: 2, z: 4, core: 2. Of those that a mesh axis runs over, the one named last changes fastest.
Arguments:
- tokens: bfloat16 [4096, 2048], P(('dp', 'expert')), may hold values from -6 to 6
- routes: int32 [4096, 8], P(('dp', 'expert')), may hold values from 0 to 15, all different within a row
- route_weight: float32 [4096, 8], P(('dp', 'expert')), may hold values from 0.05 to 0.5
- bias: float32 [16], replicated, may hold values from -3 to 3
- w_gate: bfloat16 [16, 768, 2048], P('expert', 'dp'), may hold values from -0.125 to 0.125
- w_up: bfloat16 [16, 768, 2048], P('expert', 'dp'), may hold values from -0.125 to 0.125
- w_down: bfloat16 [16, 768, 2048], P('expert', 'dp'), may hold values from -0.21875 to 0.21875
Outputs:
- mixed: bfloat16 [4096, 2048], P(('dp', 'expert'))
- new_bias: float32 [16], replicated
- counts: int32 [16], replicated
The draws below stay inside these ranges and needn't reach their ends.
Inputs may be any that keep to these rules, and one draw needn't show every extreme that they name: `routes`: each token names 8 different experts.
All inputs are finite; a program needn't handle non-finite values.
Results may differ from the reference program's by a relative error of at most 0.0057.
Values may be sent and summed in bfloat16 or wider, within the bound.
A program may use at most 128 MiB of HBM per device.

```python
import jax
import jax.numpy as jnp
from jax import lax

D = 2048
FF = 768
TOP = 8
TOK_DEV = 128
EXPERTS = 16
TOKENS = 4096
CAP = 80


def level_of(rng, extent, shards, smallest, top_value):
    loudness, own = 1.0, jax.random.fold_in(rng, 6)
    for position, shards_of in shards:
        heights = jnp.exp(jax.random.uniform(jax.random.fold_in(own, position), (shards_of,), jnp.float32, smallest / len(shards), top_value / len(shards)))
        loudness = loudness * jnp.repeat(heights, extent[position] // shards_of).reshape([-1 if axis == position else 1 for axis in range(len(extent))])
    return loudness


def different_ones(key, rows, amount, top, lift):
    order = jax.random.permutation(jax.random.fold_in(key, 1), amount)
    favour = order
    for power in range(3):
        favour = favour * favour // amount
    favour = favour * lift // amount
    lots = jax.random.randint(jax.random.fold_in(key, 2), (rows, amount), 0, 4096) + favour
    holders = jax.random.permutation(jax.random.fold_in(key, 3), rows)[jnp.arange(amount) % rows]
    lots = jnp.where(jnp.arange(rows)[:, None] == holders[None, :], 1 << 14, lots)
    merit = lots * amount + jnp.arange(amount)
    return lax.top_k(merit.astype(jnp.int32), top)[1].astype(jnp.int32)


def scatter_about(own_key, extent, width, reach, shards=(), held_as=jnp.bfloat16):
    drawn = jax.random.normal(own_key, extent, jnp.float32) * width
    if len(shards) > 0:
        drawn = level_of(own_key, extent, shards, -0.22, 0.18) * drawn
    return jnp.clip(drawn, min=-reach, max=reach).astype(held_as)


def setup_inputs(seed: int = 0) -> dict:
    key_of = jax.random.split(jax.random.key(seed), 8)
    tokens = scatter_about(key_of[0], (TOKENS, D), 1.0, 6.0, ((0, 32),))
    routes = different_ones(key_of[1], TOKENS, EXPERTS, TOP, 4096)
    route_weight = jnp.clip(0.05 + 0.45 * jax.random.uniform(key_of[2], (TOKENS, TOP), jnp.float32) ** level_of(key_of[2], (TOKENS, TOP), ((0, 32),), -0.2, 0.2), 0.05, 0.5)
    bias = scatter_about(key_of[3], (EXPERTS,), 0.5, 3.0, (), jnp.float32)
    w_gate = scatter_about(key_of[4], (EXPERTS, FF, D), D ** -0.5, 0.125, ((0, 8), (1, 4)))
    w_up = scatter_about(key_of[5], (EXPERTS, FF, D), D ** -0.5, 0.125, ((0, 8), (1, 4)))
    w_down = scatter_about(key_of[6], (EXPERTS, FF, D), FF ** -0.5, 0.21875, ((0, 8), (1, 4)))
    return dict(tokens=tokens, routes=routes, route_weight=route_weight, bias=bias, w_gate=w_gate, w_up=w_up, w_down=w_down)


bias_rate = 0.05


def reference(tokens, routes, route_weight, bias, w_gate, w_up, w_down):
    sources = TOKENS // TOK_DEV
    entries = TOK_DEV * TOP
    block_routes = routes.reshape(sources, entries)
    labels = jnp.arange(EXPERTS, dtype=jnp.int32)

    def rank_block(block_row):
        picked = (block_row[:, None] == labels[None, :]).astype(jnp.int32)
        running = jnp.cumsum(picked, axis=0) - picked
        return jnp.sum(running * picked, axis=1).astype(jnp.int32), jnp.sum(picked, axis=0).astype(jnp.int32)

    slot_rank, block_counts = lax.map(rank_block, block_routes)
    counts = jnp.sum(block_counts, axis=0).astype(jnp.int32)
    kept_mask = slot_rank < CAP
    source_index = jnp.arange(sources, dtype=jnp.int32)[:, None]
    token_index = (source_index * TOK_DEV + jnp.arange(entries, dtype=jnp.int32)[None, :] // TOP).astype(jnp.int32)
    slot_total = EXPERTS * sources * CAP
    slot_index = jnp.where(kept_mask, block_routes * (sources * CAP) + source_index * CAP + slot_rank, slot_total).astype(jnp.int32)
    token_table = jnp.zeros((slot_total + 1,), jnp.int32).at[slot_index.reshape(-1)].set(token_index.reshape(-1))
    token_table = token_table[:slot_total].reshape(EXPERTS, sources * CAP)
    entry_weight = jnp.where(kept_mask, route_weight.reshape(sources, entries), jnp.float32(0.0)).astype(jnp.float32)
    weight_table = jnp.zeros((slot_total + 1,), jnp.float32).at[slot_index.reshape(-1)].set(entry_weight.reshape(-1))
    weight_table = weight_table[:slot_total].reshape(EXPERTS, sources * CAP)

    def one_expert(carry_sum, expert_items):
        slot_tokens, slot_weights, gate_w, up_w, down_w = expert_items
        picked_rows = tokens[slot_tokens]
        gate_act = lax.dot_general(picked_rows, gate_w, (((1,), (1,)), ((), ())), preferred_element_type=jnp.float32)
        up_act = lax.dot_general(picked_rows, up_w, (((1,), (1,)), ((), ())), preferred_element_type=jnp.float32)
        hidden = (jax.nn.silu(gate_act) * up_act).astype(jnp.bfloat16)
        expert_out = jnp.dot(hidden, down_w, preferred_element_type=jnp.float32).astype(jnp.bfloat16)
        return carry_sum.at[slot_tokens].add(expert_out.astype(jnp.float32) * slot_weights[:, None]), None

    summed, _ = lax.scan(one_expert, jnp.zeros((TOKENS, D), jnp.float32), (token_table, weight_table, w_gate, w_up, w_down))
    mixed = summed.astype(jnp.bfloat16)
    new_bias = bias + bias_rate * jnp.sign((TOKENS * TOP - EXPERTS * counts).astype(jnp.float32))
    return mixed, new_bias, counts
```

```python
import functools

import jax
import jax.numpy as jnp
from jax import lax
from jax.experimental import pallas as pl
from jax.experimental.pallas import tpu as pltpu
from jax.sharding import PartitionSpec as P

bias_rate = 0.05
MESH = pl.DeviceIdType.MESH
VMEM_BYTES = 67043328
chunks = 4


def expert_products(received, gate_w, up_w, down_w):
    gate_act = jnp.einsum("sjcd,jfd->sjcf", received, gate_w, preferred_element_type=jnp.float32)
    up_act = jnp.einsum("sjcd,jfd->sjcf", received, up_w, preferred_element_type=jnp.float32)
    hidden = (jax.nn.silu(gate_act) * up_act).astype(jnp.bfloat16)
    return jnp.einsum("sjcf,jfd->sjcd", hidden, down_w, preferred_element_type=jnp.float32)


def exchange_body(tokens, routes, route_weight, bias, w_gate, w_up, w_down):
    tok_rows, feature_width = tokens.shape
    top_count = routes.shape[1]
    experts = bias.shape[0]
    groups = lax.axis_size("expert")
    per_device = w_gate.shape[0]
    capacity = 5 * tok_rows * top_count // (4 * experts)
    flat_routes = routes.reshape(-1)
    labels = jnp.arange(experts, dtype=jnp.int32)
    picked = (flat_routes[:, None] == labels[None, :]).astype(jnp.int32)
    running = jnp.cumsum(picked, axis=0) - picked
    slot_rank = jnp.sum(running * picked, axis=1)
    local_counts = jnp.sum(picked, axis=0)
    kept_mask = slot_rank < capacity
    slot_total = experts * capacity
    slot_index = jnp.where(kept_mask, flat_routes * capacity + slot_rank, slot_total)
    token_index = jnp.arange(tok_rows * top_count, dtype=jnp.int32) // top_count
    source = jnp.zeros((slot_total + 1,), jnp.int32).at[slot_index].set(token_index)[:slot_total]
    filled = jnp.zeros((slot_total + 1,), jnp.bool_).at[slot_index].set(True)[:slot_total]
    send_rows = jnp.where(filled[:, None], tokens[source], jnp.zeros((), jnp.bfloat16))
    send_rows = send_rows.reshape(groups, per_device, capacity, feature_width)
    gathered = [lax.all_gather(w, "dp", axis=1, tiled=True) for w in (w_gate, w_up, w_down)]
    produced = expert_products(
        lax.all_to_all(send_rows, "expert", split_axis=0, concat_axis=0, tiled=True), *gathered
    ).astype(jnp.bfloat16)
    returned = lax.all_to_all(produced, "expert", split_axis=0, concat_axis=0, tiled=True)
    flat_out = returned.reshape(slot_total, feature_width)
    fetched = flat_out[jnp.minimum(slot_index, slot_total - 1)]
    entry_weight = jnp.where(kept_mask, route_weight.reshape(-1), jnp.float32(0.0))
    weighted = fetched.astype(jnp.float32) * entry_weight[:, None]
    mixed = jnp.sum(weighted.reshape(tok_rows, top_count, feature_width), axis=1).astype(
        jnp.bfloat16
    )
    mean_load = tok_rows * top_count * lax.axis_size("dp") * groups
    totals = lax.psum(local_counts.astype(jnp.float32), ("dp", "expert"))
    new_bias = bias + bias_rate * jnp.sign(mean_load - experts * totals)
    return (mixed, new_bias, totals.astype(jnp.int32))


def layer_kernel(
    zs, capacity, per_device,
    tokens, routes_t, weights_t, w_gate, w_up, w_down,
    out, totals,
    tok, table, gate_w, up_w, down_own, down_far, hidden,
    part1, recv1, part2, recv2, part3, recv3, tally, tally_in,
    tok_in, tok_out, tab_in, tab_out, own_sem, w_in, w_out, d_in, d_out,
    s1_in, s1_out, s2_in, s2_out, s3_in, s3_out, t_in, t_out,
):
    rows, width = tokens.shape
    top = routes_t.shape[0]
    experts = table.shape[1] // 2
    ff = w_gate.shape[0]
    unit = ff // per_device
    cd = width // chunks
    slots = tok.shape[0]
    dp, ex = lax.axis_index("dp"), lax.axis_index("expert")
    y, x = dp // 2, dp % 2
    z, c = ex // 2, ex % 2

    def at(y_, x_, z_, c_):
        return (y_ * 2 + x_, z_ * 2 + c_)

    def slot(y_, z_, c_):
        return (y_ * zs + z_) * 2 + c_

    def far(step):
        return lax.rem(z + step, zs)

    mate = at(y, x, z, 1 - c)
    y_side = at(1 - y, x, z, c)
    x_side = at(y, 1 - x, z, c)
    me = slot(y, z, c)

    barrier = pltpu.get_barrier_semaphore()
    partners = [mate, y_side, x_side] + [at(y, x, far(s), c) for s in range(1, zs)]
    for partner in partners:
        pl.semaphore_signal(barrier, inc=1, device_id=partner, device_id_type=MESH)

    own = [
        pltpu.make_async_copy(tokens, tok.at[me], own_sem.at[0]),
        pltpu.make_async_copy(w_gate, gate_w.at[0], own_sem.at[1]),
        pltpu.make_async_copy(w_up, up_w.at[0], own_sem.at[2]),
        pltpu.make_async_copy(w_down, down_own, own_sem.at[3]),
    ]
    for copy in own:
        copy.start()

    labels = lax.broadcasted_iota(jnp.int32, (experts, rows), 0)
    picked = jnp.zeros((experts, rows), jnp.float32)
    weight = jnp.zeros((experts, rows), jnp.float32)
    for k in range(top):
        same = labels == routes_t[k : k + 1, :]
        picked += jnp.where(same, 1.0, 0.0)
        weight += jnp.where(same, weights_t[k : k + 1, :], 0.0)
    earlier = jnp.where(
        lax.broadcasted_iota(jnp.int32, (rows, rows), 0)
        < lax.broadcasted_iota(jnp.int32, (rows, rows), 1),
        1.0,
        0.0,
    )
    rank = jnp.dot(
        picked.astype(jnp.bfloat16),
        earlier.astype(jnp.bfloat16),
        preferred_element_type=jnp.float32,
    )
    table[me, 0:experts, :] = jnp.where(rank < capacity, weight, 0.0)
    table[me, experts : 2 * experts, :] = picked

    pl.semaphore_wait(barrier, len(partners))

    sent = []

    def remote(src, dst, ssem, rsem, device):
        copy = pltpu.make_async_remote_copy(
            src_ref=src, dst_ref=dst, send_sem=ssem, recv_sem=rsem,
            device_id=device, device_id_type=MESH,
        )
        copy.start()
        sent.append(copy)

    def landed(ref, sem):
        pltpu.make_async_copy(ref, ref, sem).wait()

    order = [0]

    def pass_on(index, device, first=False):
        n = order[0]
        order[0] += 1
        remote(table.at[index], table.at[index], tab_out.at[n], tab_in.at[index], device)
        remote(
            tokens if first else tok.at[index], tok.at[index],
            tok_out.at[n], tok_in.at[index], device,
        )

    def arrived(index):
        landed(table.at[index], tab_in.at[index])
        landed(tok.at[index], tok_in.at[index])

    remote(w_gate, gate_w.at[1], w_out.at[0], w_in.at[0], x_side)
    remote(w_up, up_w.at[1], w_out.at[1], w_in.at[1], x_side)
    pass_on(me, y_side, True)
    for s in range(1, zs):
        pass_on(me, at(y, x, far(s), c), True)
    pass_on(me, mate, True)
    for j in range(chunks):
        remote(
            w_down.at[:, j * cd : (j + 1) * cd], down_far.at[j], d_out.at[j], d_in.at[j], x_side
        )
    for copy in own:
        copy.wait()

    def scales(index):
        columns = []
        for j in range(per_device):
            row = table[index, pl.ds(ex * per_device + j, 1), :]
            columns.append(jnp.transpose(jnp.broadcast_to(row, (rows, rows))))
        lanes = columns[0].shape[1]
        place = lax.broadcasted_iota(jnp.int32, (rows, lanes), 1)
        pieces = []
        for t in range(ff // lanes):
            piece = columns[0]
            for j in range(1, per_device):
                piece = jnp.where(place + t * lanes >= j * unit, columns[j], piece)
            pieces.append(piece)
        return jnp.concatenate(pieces, axis=1)

    nt = (((1,), (1,)), ((), ()))

    def hide(first, count, half):
        block = tok[pl.ds(first, count)].reshape(count * rows, width)
        gate = lax.dot_general(block, gate_w[half], nt, preferred_element_type=jnp.float32)
        up = lax.dot_general(block, up_w[half], nt, preferred_element_type=jnp.float32)
        act = gate / (1.0 + jnp.exp(-gate)) * up
        for i in range(count):
            value = act[i * rows : (i + 1) * rows] * scales(first + i)
            hidden[first + i, :, half * ff : (half + 1) * ff] = value.astype(jnp.bfloat16)

    def pair(y_, z_):
        arrived(slot(y_, z_, 1 - c))
        hide(slot(y_, z_, 0), 2, 0)

    arrived(slot(1 - y, z, c))
    pass_on(slot(1 - y, z, c), mate)
    for s in range(1, zs):
        from_z = lax.rem(z + zs - s, zs)
        arrived(slot(y, from_z, c))
        pass_on(slot(y, from_z, c), y_side)
        pass_on(slot(y, from_z, c), mate)
        if s == 1:
            pair(y, z)
            pair(1 - y, z)
        else:
            pair(y, lax.rem(z + zs - s + 1, zs))
    pair(y, lax.rem(z + 1, zs))
    for s in range(1, zs):
        from_z = lax.rem(z + zs - s, zs)
        arrived(slot(1 - y, from_z, c))
        pass_on(slot(1 - y, from_z, c), mate)
        if s > 1:
            pair(1 - y, lax.rem(z + zs - s + 1, zs))
    pair(1 - y, lax.rem(z + 1, zs))

    def add_tally(i, total):
        return total + table[i, experts : 2 * experts, :]

    tally[...] = lax.fori_loop(0, slots, add_tally, jnp.zeros((experts, rows), jnp.float32))

    landed(gate_w.at[1], w_in.at[0])
    landed(up_w.at[1], w_in.at[1])
    remote(tally, tally_in, t_out, t_in, x_side)

    batch = 4

    def other_half(q, carry):
        hide(q * batch, batch, 1)
        return carry

    lax.fori_loop(0, slots // batch, other_half, 0)

    def down(j):
        landed(down_far.at[j], d_in.at[j])

        def step(q, carry):
            near = hidden[pl.ds(q * batch, batch)].reshape(batch * rows, 2 * ff)
            value = jnp.dot(
                near[:, :ff], down_own[:, j * cd : (j + 1) * cd],
                preferred_element_type=jnp.float32,
            ) + jnp.dot(near[:, ff:], down_far[j], preferred_element_type=jnp.float32)
            value = value.astype(jnp.bfloat16)
            for i in range(batch):
                part1[j, i % 2, q * (batch // 2) + i // 2] = value[i * rows : (i + 1) * rows]
            return carry

        lax.fori_loop(0, slots // batch, step, 0)
        remote(part1.at[j, 1 - c], recv1.at[j], s1_out.at[j], s1_in.at[j], mate)

    def over_core(j):
        landed(recv1.at[j], s1_in.at[j])

        def step(i, carry):
            value = part1[j, c, i].astype(jnp.float32) + recv1[j, i].astype(jnp.float32)
            part2[j, i] = value.astype(jnp.bfloat16)
            return carry

        lax.fori_loop(0, slots // 2, step, 0)
        remote(
            part2.at[j, pl.ds((1 - y) * zs, zs)], recv2.at[j], s2_out.at[j], s2_in.at[j], y_side
        )

    def over_y(j):
        landed(recv2.at[j], s2_in.at[j])

        def step(i, carry):
            value = part2[j, y * zs + i].astype(jnp.float32) + recv2[j, i].astype(jnp.float32)
            part3[j, i] = value.astype(jnp.bfloat16)
            return carry

        lax.fori_loop(0, zs, step, 0)
        for s in range(1, zs):
            remote(
                part3.at[j, far(s)], recv3.at[j, s - 1],
                s3_out.at[j, s - 1], s3_in.at[j, s - 1], at(y, x, far(s), c),
            )

    def over_z(j):
        value = part3[j, z].astype(jnp.float32)
        for s in range(1, zs):
            landed(recv3.at[j, s - 1], s3_in.at[j, s - 1])
            value += recv3[j, s - 1].astype(jnp.float32)
        out[:, j * cd : (j + 1) * cd] = value.astype(jnp.bfloat16)

    for j in range(chunks + 3):
        if j < chunks:
            down(j)
        if 0 <= j - 1 < chunks:
            over_core(j - 1)
        if 0 <= j - 2 < chunks:
            over_y(j - 2)
        if 0 <= j - 3 < chunks:
            over_z(j - 3)

    landed(tally_in, t_in)
    count = jnp.sum(tally[...] + tally_in[...], axis=1, keepdims=True)
    totals[...] = jnp.broadcast_to(count, totals.shape)
    for copy in sent:
        copy.wait_send()


def group_scratch(zs, rows, width, ff, experts):
    slots = 4 * zs
    cd = width // chunks
    bf, f32 = jnp.bfloat16, jnp.float32
    return [
        ((slots, rows, width), bf),
        ((slots, 2 * experts, rows), f32),
        ((2, ff, width), bf),
        ((2, ff, width), bf),
        ((ff, width), bf),
        ((chunks, ff, cd), bf),
        ((slots, rows, 2 * ff), bf),
        ((chunks, 2, slots // 2, rows, cd), bf),
        ((chunks, slots // 2, rows, cd), bf),
        ((chunks, slots // 2, rows, cd), bf),
        ((chunks, zs, rows, cd), bf),
        ((chunks, zs, rows, cd), bf),
        ((chunks, zs - 1, rows, cd), bf),
        ((experts, rows), f32),
        ((experts, rows), f32),
    ]


def group_body(zs, tokens, routes, route_weight, bias, w_gate, w_up, w_down):
    rows, width = tokens.shape
    experts = bias.shape[0]
    per_device, unit, _ = w_gate.shape
    ff = per_device * unit
    top = routes.shape[1]
    capacity = 5 * rows * top // (4 * experts)
    slots = 4 * zs
    dma = pltpu.SemaphoreType.DMA
    vmem = pl.BlockSpec(memory_space=pltpu.VMEM)
    anywhere = pl.BlockSpec(memory_space=pl.ANY)
    mixed, totals = pl.pallas_call(
        functools.partial(layer_kernel, zs, capacity, per_device),
        out_shape=(
            jax.ShapeDtypeStruct((rows, width), jnp.bfloat16),
            jax.ShapeDtypeStruct((experts, rows), jnp.float32),
        ),
        in_specs=[anywhere, vmem, vmem, anywhere, anywhere, anywhere],
        out_specs=(vmem, vmem),
        scratch_shapes=[
            pltpu.VMEM(shape, kind)
            for shape, kind in group_scratch(zs, rows, width, ff, experts)
        ]
        + [
            dma((slots,)), dma((slots,)), dma((slots,)), dma((slots,)), dma((4,)),
            dma((2,)), dma((2,)), dma((chunks,)), dma((chunks,)),
            dma((chunks,)), dma((chunks,)), dma((chunks,)), dma((chunks,)),
            dma((chunks, zs - 1)), dma((chunks, zs - 1)), dma, dma,
        ],
        compiler_params=pltpu.CompilerParams(
            collective_id=0, has_side_effects=True, vmem_limit_bytes=VMEM_BYTES
        ),
    )(
        tokens, routes.T, route_weight.T,
        w_gate.reshape(ff, width), w_up.reshape(ff, width), w_down.reshape(ff, width),
    )
    counts = totals[:, 0]
    mean_load = rows * top * lax.axis_size("dp") * lax.axis_size("expert")
    new_bias = bias + bias_rate * jnp.sign(mean_load - experts * counts)
    return (mixed, new_bias, counts.astype(jnp.int32))


def body(tokens, routes, route_weight, bias, w_gate, w_up, w_down):
    rows, width = tokens.shape
    per_device, unit, _ = w_gate.shape
    groups = lax.axis_size("expert")
    zs = groups // 2
    held = group_scratch(zs, rows, width, per_device * unit, bias.shape[0])
    total = 0
    for shape, kind in held:
        size = jnp.dtype(kind).itemsize
        for extent in shape:
            size *= extent
        total += size
    args = (tokens, routes, route_weight, bias, w_gate, w_up, w_down)
    if lax.axis_size("dp") == 4 and groups % 2 == 0 and zs > 1 and total < 0.85 * VMEM_BYTES:
        return group_body(zs, *args)
    return exchange_body(*args)


def solution(mesh):
    placed = (
        P(("dp", "expert"), None),
        P(("dp", "expert"), None),
        P(("dp", "expert"), None),
        P(),
        P("expert", "dp", None),
        P("expert", "dp", None),
        P("expert", "dp", None),
    )
    return jax.shard_map(
        body,
        mesh=mesh,
        in_specs=placed,
        out_specs=(P(("dp", "expert"), None), P(), P()),
        check_vma=False,
    )
```

```python
import functools

import jax
import jax.numpy as jnp
from jax import lax
from jax.experimental import pallas as pl
from jax.experimental.pallas import tpu as pltpu
from jax.sharding import PartitionSpec as P

bias_rate = 0.05
MESH = pl.DeviceIdType.MESH
VMEM_BYTES = 67043328
chunks = 8


def expert_products(received, gate_w, up_w, down_w):
    gate_act = jnp.einsum("sjcd,jfd->sjcf", received, gate_w, preferred_element_type=jnp.float32)
    up_act = jnp.einsum("sjcd,jfd->sjcf", received, up_w, preferred_element_type=jnp.float32)
    hidden = (jax.nn.silu(gate_act) * up_act).astype(jnp.bfloat16)
    return jnp.einsum("sjcf,jfd->sjcd", hidden, down_w, preferred_element_type=jnp.float32)


def exchange_body(tokens, routes, route_weight, bias, w_gate, w_up, w_down):
    tok_rows, feature_width = tokens.shape
    top_count = routes.shape[1]
    experts = bias.shape[0]
    groups = lax.axis_size("expert")
    per_device = w_gate.shape[0]
    capacity = 5 * tok_rows * top_count // (4 * experts)
    flat_routes = routes.reshape(-1)
    labels = jnp.arange(experts, dtype=jnp.int32)
    picked = (flat_routes[:, None] == labels[None, :]).astype(jnp.int32)
    running = jnp.cumsum(picked, axis=0) - picked
    slot_rank = jnp.sum(running * picked, axis=1)
    local_counts = jnp.sum(picked, axis=0)
    kept_mask = slot_rank < capacity
    slot_total = experts * capacity
    slot_index = jnp.where(kept_mask, flat_routes * capacity + slot_rank, slot_total)
    token_index = jnp.arange(tok_rows * top_count, dtype=jnp.int32) // top_count
    source = jnp.zeros((slot_total + 1,), jnp.int32).at[slot_index].set(token_index)[:slot_total]
    filled = jnp.zeros((slot_total + 1,), jnp.bool_).at[slot_index].set(True)[:slot_total]
    send_rows = jnp.where(filled[:, None], tokens[source], jnp.zeros((), jnp.bfloat16))
    send_rows = send_rows.reshape(groups, per_device, capacity, feature_width)
    gathered = [lax.all_gather(w, "dp", axis=1, tiled=True) for w in (w_gate, w_up, w_down)]
    produced = expert_products(
        lax.all_to_all(send_rows, "expert", split_axis=0, concat_axis=0, tiled=True), *gathered
    ).astype(jnp.bfloat16)
    returned = lax.all_to_all(produced, "expert", split_axis=0, concat_axis=0, tiled=True)
    flat_out = returned.reshape(slot_total, feature_width)
    fetched = flat_out[jnp.minimum(slot_index, slot_total - 1)]
    entry_weight = jnp.where(kept_mask, route_weight.reshape(-1), jnp.float32(0.0))
    weighted = fetched.astype(jnp.float32) * entry_weight[:, None]
    mixed = jnp.sum(weighted.reshape(tok_rows, top_count, feature_width), axis=1).astype(
        jnp.bfloat16
    )
    mean_load = tok_rows * top_count * lax.axis_size("dp") * groups
    totals = lax.psum(local_counts.astype(jnp.float32), ("dp", "expert"))
    new_bias = bias + bias_rate * jnp.sign(mean_load - experts * totals)
    return (mixed, new_bias, totals.astype(jnp.int32))


def layer_kernel(
    zs, capacity, per_device,
    tokens, routes_t, weights_t, w_gate, w_up, w_down,
    out, totals,
    tok, table, gate_w, up_w, down_own, down_far, hidden,
    part1, keep1, recv1, part2, keep2, recv2, part3, keep3, recv3, tally, tally_in,
    tok_in, tok_out, tab_in, tab_out, own_sem, w_in, w_out, d_in, d_out,
    s1_in, s1_out, s2_in, s2_out, s3_in, s3_out, t_in, t_out,
):
    rows, width = tokens.shape
    top = routes_t.shape[0]
    experts = table.shape[1] // 2
    ff = w_gate.shape[0]
    unit = ff // per_device
    cd = width // chunks
    slots = tok.shape[0]
    dp, ex = lax.axis_index("dp"), lax.axis_index("expert")
    y, x = dp // 2, dp % 2
    z, c = ex // 2, ex % 2

    def at(y_, x_, z_, c_):
        return (y_ * 2 + x_, z_ * 2 + c_)

    def slot(y_, z_, c_):
        return (y_ * zs + z_) * 2 + c_

    def far(step):
        return lax.rem(z + step, zs)

    mate = at(y, x, z, 1 - c)
    y_side = at(1 - y, x, z, c)
    x_side = at(y, 1 - x, z, c)
    me = slot(y, z, c)

    barrier = pltpu.get_barrier_semaphore()
    partners = [mate, y_side, x_side] + [at(y, x, far(s), c) for s in range(1, zs)]
    for partner in partners:
        pl.semaphore_signal(barrier, inc=1, device_id=partner, device_id_type=MESH)

    own = [
        pltpu.make_async_copy(tokens, tok.at[me], own_sem.at[0]),
        pltpu.make_async_copy(w_gate, gate_w.at[0], own_sem.at[1]),
        pltpu.make_async_copy(w_up, up_w.at[0], own_sem.at[2]),
        pltpu.make_async_copy(w_down, down_own, own_sem.at[3]),
    ]
    for copy in own:
        copy.start()

    labels = lax.broadcasted_iota(jnp.int32, (experts, rows), 0)
    picked = jnp.zeros((experts, rows), jnp.float32)
    weight = jnp.zeros((experts, rows), jnp.float32)
    for k in range(top):
        same = labels == routes_t[k : k + 1, :]
        picked += jnp.where(same, 1.0, 0.0)
        weight += jnp.where(same, weights_t[k : k + 1, :], 0.0)
    earlier = jnp.where(
        lax.broadcasted_iota(jnp.int32, (rows, rows), 0)
        < lax.broadcasted_iota(jnp.int32, (rows, rows), 1),
        1.0,
        0.0,
    )
    rank = jnp.dot(
        picked.astype(jnp.bfloat16),
        earlier.astype(jnp.bfloat16),
        preferred_element_type=jnp.float32,
    )
    table[me, 0:experts, :] = jnp.where(rank < capacity, weight, 0.0)
    table[me, experts : 2 * experts, :] = picked

    pl.semaphore_wait(barrier, len(partners))

    sent = []

    def remote(src, dst, ssem, rsem, device, keep=True):
        copy = pltpu.make_async_remote_copy(
            src_ref=src, dst_ref=dst, send_sem=ssem, recv_sem=rsem,
            device_id=device, device_id_type=MESH,
        )
        copy.start()
        if keep:
            sent.append(copy)

    def landed(ref, sem):
        pltpu.make_async_copy(ref, ref, sem).wait()

    def pass_on(n, index, device, source=None):
        remote(table.at[index], table.at[index], tab_out.at[n], tab_in.at[index], device, False)
        remote(
            tok.at[index] if source is None else source, tok.at[index],
            tok_out.at[n], tok_in.at[index], device, False,
        )

    def passed(n):
        pltpu.make_async_copy(table.at[0], table.at[0], tab_out.at[n]).wait()
        pltpu.make_async_copy(tok.at[0], tok.at[0], tok_out.at[n]).wait()

    def arrived(index):
        landed(table.at[index], tab_in.at[index])
        landed(tok.at[index], tok_in.at[index])

    above, below = z < zs - 1, z > 0
    z_up, z_down = at(y, x, z + 1, c), at(y, x, z - 1, c)

    for j in range(per_device):
        units = pl.ds(j * unit, unit)
        remote(w_gate.at[units], gate_w.at[1, units], w_out.at[0, j], w_in.at[0, j], x_side)
        remote(w_up.at[units], up_w.at[1, units], w_out.at[1, j], w_in.at[1, j], x_side)
    @pl.when(above)
    def _():
        pass_on(z, me, z_up, tokens)

    @pl.when(below)
    def _():
        pass_on(zs + z, me, z_down, tokens)

    pass_on(2 * zs + z, me, y_side, tokens)
    pass_on(3 * zs + me // 2, me, mate, tokens)
    for j in range(chunks):
        remote(
            w_down.at[:, j * cd : (j + 1) * cd], down_far.at[j], d_out.at[j], d_in.at[j], x_side
        )
    for copy in own:
        copy.wait()

    def column(index, j):
        row = table[index, pl.ds(ex * per_device + j, 1), :]
        return jnp.transpose(jnp.broadcast_to(row, (rows, rows)))

    def scales(index):
        columns = [column(index, j) for j in range(per_device)]
        lanes = columns[0].shape[1]
        place = lax.broadcasted_iota(jnp.int32, (rows, lanes), 1)
        pieces = []
        for t in range(ff // lanes):
            piece = columns[0]
            for j in range(1, per_device):
                piece = jnp.where(place + t * lanes >= j * unit, columns[j], piece)
            pieces.append(piece)
        return jnp.concatenate(pieces, axis=1)

    nt = (((1,), (1,)), ((), ()))

    def act(block, gate_t, up_t):
        gate = lax.dot_general(block, gate_t, nt, preferred_element_type=jnp.float32)
        up = lax.dot_general(block, up_t, nt, preferred_element_type=jnp.float32)
        return gate / (1.0 + jnp.exp(-gate)) * up

    batch = 4

    def relay(source, onward, device, n):
        index = slot(y, source, c)
        arrived(index)

        @pl.when(onward)
        def _():
            pass_on(n + source, index, device)

        pass_on(2 * zs + source, index, y_side)
        pass_on(3 * zs + index // 2, index, mate)

    for d in range(1, zs):

        @pl.when(z >= d)
        def _():
            relay(z - d, above, z_up, 0)

        @pl.when(z + d < zs)
        def _():
            relay(z + d, below, z_down, zs)

    def from_y(source):
        index = slot(1 - y, source, c)
        arrived(index)
        pass_on(3 * zs + index // 2, index, mate)

    from_y(z)
    for d in range(1, zs):

        @pl.when(z >= d)
        def _():
            from_y(z - d)

        @pl.when(z + d < zs)
        def _():
            from_y(z + d)

    def from_mate(i, carry):
        arrived(2 * i + 1 - c)
        return carry

    lax.fori_loop(0, slots // 2, from_mate, 0)

    def own_half(q, carry):
        first = q * batch
        block = tok[pl.ds(first, batch)].reshape(batch * rows, width)
        value = act(block, gate_w[0], up_w[0])
        for i in range(batch):
            scaled = value[i * rows : (i + 1) * rows] * scales(first + i)
            hidden[first + i, :, 0:ff] = scaled.astype(jnp.bfloat16)
        return carry

    lax.fori_loop(0, slots // batch, own_half, 0)

    def add_tally(i, total):
        return total + table[i, experts : 2 * experts, :]

    tally[...] = lax.fori_loop(0, slots, add_tally, jnp.zeros((experts, rows), jnp.float32))

    remote(tally, tally_in, t_out, t_in, x_side)

    for j in range(per_device):
        units = pl.ds(j * unit, unit)
        landed(gate_w.at[1, units], w_in.at[0, j])
        landed(up_w.at[1, units], w_in.at[1, j])

        def other_half(q, carry):
            first = q * batch
            block = tok[pl.ds(first, batch)].reshape(batch * rows, width)
            value = act(block, gate_w[1, j * unit : (j + 1) * unit], up_w[1, j * unit : (j + 1) * unit])
            for i in range(batch):
                scaled = value[i * rows : (i + 1) * rows] * column(first + i, j)[:, 0:1]
                hidden[first + i, :, ff + j * unit : ff + (j + 1) * unit] = scaled.astype(
                    jnp.bfloat16
                )
            return carry

        lax.fori_loop(0, slots // batch, other_half, 0)

    def down(j):
        landed(down_far.at[j], d_in.at[j])

        def step(q, carry):
            near = hidden[pl.ds(q * batch, batch)].reshape(batch * rows, 2 * ff)
            value = jnp.dot(
                near[:, :ff], down_own[:, j * cd : (j + 1) * cd],
                preferred_element_type=jnp.float32,
            ) + jnp.dot(near[:, ff:], down_far[j], preferred_element_type=jnp.float32)
            for i in range(batch // 2):
                one = value[2 * i * rows : (2 * i + 1) * rows]
                two = value[(2 * i + 1) * rows : (2 * i + 2) * rows]
                keep1[j, q * (batch // 2) + i] = jnp.where(c == 0, one, two)
                part1[j, q * (batch // 2) + i] = jnp.where(c == 0, two, one).astype(jnp.bfloat16)
            return carry

        lax.fori_loop(0, slots // batch, step, 0)
        remote(part1.at[j], recv1.at[j], s1_out.at[j], s1_in.at[j], mate)

    def over_core(j):
        landed(recv1.at[j], s1_in.at[j])

        def away(i, carry):
            n = (1 - y) * zs + i
            value = keep1[j, n] + recv1[j, n].astype(jnp.float32)
            part2[j, i] = value.astype(jnp.bfloat16)
            return carry

        lax.fori_loop(0, zs, away, 0)
        remote(part2.at[j], recv2.at[j], s2_out.at[j], s2_in.at[j], y_side)

        def home(i, carry):
            n = y * zs + i
            keep2[j, i] = keep1[j, n] + recv1[j, n].astype(jnp.float32)
            return carry

        lax.fori_loop(0, zs, home, 0)

    def over_y(j):
        landed(recv2.at[j], s2_in.at[j])

        for s in range(1, zs):
            n = far(s)
            value = keep2[j, n] + recv2[j, n].astype(jnp.float32)
            part3[j, s - 1] = value.astype(jnp.bfloat16)
            remote(
                part3.at[j, s - 1], recv3.at[j, s - 1],
                s3_out.at[j, s - 1], s3_in.at[j, s - 1], at(y, x, n, c),
            )
        keep3[j] = keep2[j, z] + recv2[j, z].astype(jnp.float32)

    def over_z(j):
        value = keep3[j]
        for s in range(1, zs):
            landed(recv3.at[j, s - 1], s3_in.at[j, s - 1])
            value += recv3[j, s - 1].astype(jnp.float32)
        out[:, j * cd : (j + 1) * cd] = value.astype(jnp.bfloat16)

    for j in range(chunks + 3):
        if j < chunks:
            down(j)
        if 0 <= j - 1 < chunks:
            over_core(j - 1)
        if 0 <= j - 2 < chunks:
            over_y(j - 2)
        if 0 <= j - 3 < chunks:
            over_z(j - 3)

    landed(tally_in, t_in)
    count = jnp.sum(tally[...] + tally_in[...], axis=1, keepdims=True)
    totals[...] = jnp.broadcast_to(count, totals.shape)
    for copy in sent:
        copy.wait_send()

    def z_sent(source, carry):
        @pl.when(jnp.logical_and(above, source <= z))
        def _():
            passed(source)

        @pl.when(jnp.logical_and(below, source >= z))
        def _():
            passed(zs + source)

        passed(2 * zs + source)
        return carry

    lax.fori_loop(0, zs, z_sent, 0)

    def mate_sent(i, carry):
        passed(3 * zs + i)
        return carry

    lax.fori_loop(0, slots // 2, mate_sent, 0)


def group_scratch(zs, rows, width, ff, experts):
    slots = 4 * zs
    cd = width // chunks
    bf, f32 = jnp.bfloat16, jnp.float32
    return [
        ((slots, rows, width), bf),
        ((slots, 2 * experts, rows), f32),
        ((2, ff, width), bf),
        ((2, ff, width), bf),
        ((ff, width), bf),
        ((chunks, ff, cd), bf),
        ((slots, rows, 2 * ff), bf),
        ((chunks, slots // 2, rows, cd), bf),
        ((chunks, slots // 2, rows, cd), f32),
        ((chunks, slots // 2, rows, cd), bf),
        ((chunks, zs, rows, cd), bf),
        ((chunks, zs, rows, cd), f32),
        ((chunks, zs, rows, cd), bf),
        ((chunks, zs - 1, rows, cd), bf),
        ((chunks, rows, cd), f32),
        ((chunks, zs - 1, rows, cd), bf),
        ((experts, rows), f32),
        ((experts, rows), f32),
    ]


def group_body(zs, tokens, routes, route_weight, bias, w_gate, w_up, w_down):
    rows, width = tokens.shape
    experts = bias.shape[0]
    per_device, unit, _ = w_gate.shape
    ff = per_device * unit
    top = routes.shape[1]
    capacity = 5 * rows * top // (4 * experts)
    slots = 4 * zs
    dma = pltpu.SemaphoreType.DMA
    vmem = pl.BlockSpec(memory_space=pltpu.VMEM)
    anywhere = pl.BlockSpec(memory_space=pl.ANY)
    mixed, totals = pl.pallas_call(
        functools.partial(layer_kernel, zs, capacity, per_device),
        out_shape=(
            jax.ShapeDtypeStruct((rows, width), jnp.bfloat16),
            jax.ShapeDtypeStruct((experts, rows), jnp.float32),
        ),
        in_specs=[anywhere, vmem, vmem, anywhere, anywhere, anywhere],
        out_specs=(vmem, vmem),
        scratch_shapes=[
            pltpu.VMEM(shape, kind)
            for shape, kind in group_scratch(zs, rows, width, ff, experts)
        ]
        + [
            dma((slots,)), dma((5 * zs,)), dma((slots,)), dma((5 * zs,)), dma((4,)),
            dma((2, per_device)), dma((2, per_device)), dma((chunks,)), dma((chunks,)),
            dma((chunks,)), dma((chunks,)), dma((chunks,)), dma((chunks,)),
            dma((chunks, zs - 1)), dma((chunks, zs - 1)), dma, dma,
        ],
        compiler_params=pltpu.CompilerParams(
            collective_id=0, has_side_effects=True, vmem_limit_bytes=VMEM_BYTES
        ),
    )(
        tokens, routes.T, route_weight.T,
        w_gate.reshape(ff, width), w_up.reshape(ff, width), w_down.reshape(ff, width),
    )
    counts = totals[:, 0]
    mean_load = rows * top * lax.axis_size("dp") * lax.axis_size("expert")
    new_bias = bias + bias_rate * jnp.sign(mean_load - experts * counts)
    return (mixed, new_bias, counts.astype(jnp.int32))


def body(tokens, routes, route_weight, bias, w_gate, w_up, w_down):
    rows, width = tokens.shape
    per_device, unit, _ = w_gate.shape
    groups = lax.axis_size("expert")
    zs = groups // 2
    held = group_scratch(zs, rows, width, per_device * unit, bias.shape[0])
    total = 0
    for shape, kind in held:
        size = jnp.dtype(kind).itemsize
        for extent in shape:
            size *= extent
        total += size
    args = (tokens, routes, route_weight, bias, w_gate, w_up, w_down)
    if lax.axis_size("dp") == 4 and groups % 2 == 0 and zs > 1 and total < 0.85 * VMEM_BYTES:
        return group_body(zs, *args)
    return exchange_body(*args)


def solution(mesh):
    placed = (
        P(("dp", "expert"), None),
        P(("dp", "expert"), None),
        P(("dp", "expert"), None),
        P(),
        P("expert", "dp", None),
        P("expert", "dp", None),
        P("expert", "dp", None),
    )
    return jax.shard_map(
        body,
        mesh=mesh,
        in_specs=placed,
        out_specs=(P(("dp", "expert"), None), P(), P()),
        check_vma=False,
    )
```

```python
import functools

import jax
import jax.numpy as jnp
from jax import lax
from jax.experimental import pallas as pl
from jax.experimental.pallas import tpu as pltpu
from jax.sharding import PartitionSpec as P

bias_rate = 0.05
MESH = pl.DeviceIdType.MESH
VMEM_BYTES = 67043328
chunks = 8


def expert_products(received, gate_w, up_w, down_w):
    gate_act = jnp.einsum("sjcd,jfd->sjcf", received, gate_w, preferred_element_type=jnp.float32)
    up_act = jnp.einsum("sjcd,jfd->sjcf", received, up_w, preferred_element_type=jnp.float32)
    hidden = (jax.nn.silu(gate_act) * up_act).astype(jnp.bfloat16)
    return jnp.einsum("sjcf,jfd->sjcd", hidden, down_w, preferred_element_type=jnp.float32)


def exchange_body(tokens, routes, route_weight, bias, w_gate, w_up, w_down):
    tok_rows, feature_width = tokens.shape
    top_count = routes.shape[1]
    experts = bias.shape[0]
    groups = lax.axis_size("expert")
    per_device = w_gate.shape[0]
    capacity = 5 * tok_rows * top_count // (4 * experts)
    flat_routes = routes.reshape(-1)
    labels = jnp.arange(experts, dtype=jnp.int32)
    picked = (flat_routes[:, None] == labels[None, :]).astype(jnp.int32)
    running = jnp.cumsum(picked, axis=0) - picked
    slot_rank = jnp.sum(running * picked, axis=1)
    local_counts = jnp.sum(picked, axis=0)
    kept_mask = slot_rank < capacity
    slot_total = experts * capacity
    slot_index = jnp.where(kept_mask, flat_routes * capacity + slot_rank, slot_total)
    token_index = jnp.arange(tok_rows * top_count, dtype=jnp.int32) // top_count
    source = jnp.zeros((slot_total + 1,), jnp.int32).at[slot_index].set(token_index)[:slot_total]
    filled = jnp.zeros((slot_total + 1,), jnp.bool_).at[slot_index].set(True)[:slot_total]
    send_rows = jnp.where(filled[:, None], tokens[source], jnp.zeros((), jnp.bfloat16))
    send_rows = send_rows.reshape(groups, per_device, capacity, feature_width)
    gathered = [lax.all_gather(w, "dp", axis=1, tiled=True) for w in (w_gate, w_up, w_down)]
    produced = expert_products(
        lax.all_to_all(send_rows, "expert", split_axis=0, concat_axis=0, tiled=True), *gathered
    ).astype(jnp.bfloat16)
    returned = lax.all_to_all(produced, "expert", split_axis=0, concat_axis=0, tiled=True)
    flat_out = returned.reshape(slot_total, feature_width)
    fetched = flat_out[jnp.minimum(slot_index, slot_total - 1)]
    entry_weight = jnp.where(kept_mask, route_weight.reshape(-1), jnp.float32(0.0))
    weighted = fetched.astype(jnp.float32) * entry_weight[:, None]
    mixed = jnp.sum(weighted.reshape(tok_rows, top_count, feature_width), axis=1).astype(
        jnp.bfloat16
    )
    mean_load = tok_rows * top_count * lax.axis_size("dp") * groups
    totals = lax.psum(local_counts.astype(jnp.float32), ("dp", "expert"))
    new_bias = bias + bias_rate * jnp.sign(mean_load - experts * totals)
    return (mixed, new_bias, totals.astype(jnp.int32))


def layer_kernel(
    zs, capacity, per_device,
    tokens, routes_t, weights_t, w_gate, w_up, w_down,
    out, totals,
    tok, table, gate_w, up_w, down_own, down_far, hidden,
    part1, keep1, recv1, part2, keep2, recv2, part3, keep3, recv3, tally, tally_in,
    tok_in, tok_out, tab_in, tab_out, own_sem, w_in, w_out, d_in, d_out,
    s1_in, s1_out, s2_in, s2_out, s3_in, s3_out, t_in, t_out,
):
    rows, width = tokens.shape
    top = routes_t.shape[0]
    experts = table.shape[1] // 2
    ff = w_gate.shape[0]
    unit = ff // per_device
    cd = width // chunks
    slots = tok.shape[0]
    dp, ex = lax.axis_index("dp"), lax.axis_index("expert")
    y, x = dp // 2, dp % 2
    z, c = ex // 2, ex % 2

    def at(y_, x_, z_, c_):
        return (y_ * 2 + x_, z_ * 2 + c_)

    def slot(y_, z_, c_):
        return (y_ * zs + z_) * 2 + c_

    def far(step):
        return lax.rem(z + step, zs)

    mate = at(y, x, z, 1 - c)
    y_side = at(1 - y, x, z, c)
    x_side = at(y, 1 - x, z, c)
    me = slot(y, z, c)

    barrier = pltpu.get_barrier_semaphore()
    partners = [mate, y_side, x_side] + [at(y, x, far(s), c) for s in range(1, zs)]
    for partner in partners:
        pl.semaphore_signal(barrier, inc=1, device_id=partner, device_id_type=MESH)

    own = [
        pltpu.make_async_copy(tokens, tok.at[me], own_sem.at[0]),
        pltpu.make_async_copy(w_gate, gate_w.at[0], own_sem.at[1]),
        pltpu.make_async_copy(w_up, up_w.at[0], own_sem.at[2]),
        pltpu.make_async_copy(w_down, down_own, own_sem.at[3]),
    ]
    for copy in own:
        copy.start()

    labels = lax.broadcasted_iota(jnp.int32, (experts, rows), 0)
    picked = jnp.zeros((experts, rows), jnp.float32)
    weight = jnp.zeros((experts, rows), jnp.float32)
    for k in range(top):
        same = labels == routes_t[k : k + 1, :]
        picked += jnp.where(same, 1.0, 0.0)
        weight += jnp.where(same, weights_t[k : k + 1, :], 0.0)
    earlier = jnp.where(
        lax.broadcasted_iota(jnp.int32, (rows, rows), 0)
        < lax.broadcasted_iota(jnp.int32, (rows, rows), 1),
        1.0,
        0.0,
    )
    rank = jnp.dot(
        picked.astype(jnp.bfloat16),
        earlier.astype(jnp.bfloat16),
        preferred_element_type=jnp.float32,
    )
    table[me, 0:experts, :] = jnp.where(rank < capacity, weight, 0.0)
    table[me, experts : 2 * experts, :] = picked

    pl.semaphore_wait(barrier, len(partners))

    sent = []

    def remote(src, dst, ssem, rsem, device, keep=True):
        copy = pltpu.make_async_remote_copy(
            src_ref=src, dst_ref=dst, send_sem=ssem, recv_sem=rsem,
            device_id=device, device_id_type=MESH,
        )
        copy.start()
        if keep:
            sent.append(copy)

    def landed(ref, sem):
        pltpu.make_async_copy(ref, ref, sem).wait()

    def pass_on(n, index, device, source=None):
        remote(table.at[index], table.at[index], tab_out.at[n], tab_in.at[index], device, False)
        remote(
            tok.at[index] if source is None else source, tok.at[index],
            tok_out.at[n], tok_in.at[index], device, False,
        )

    def passed(n):
        pltpu.make_async_copy(table.at[0], table.at[0], tab_out.at[n]).wait()
        pltpu.make_async_copy(tok.at[0], tok.at[0], tok_out.at[n]).wait()

    def arrived(index):
        landed(table.at[index], tab_in.at[index])
        landed(tok.at[index], tok_in.at[index])

    above, below = z < zs - 1, z > 0
    z_up, z_down = at(y, x, z + 1, c), at(y, x, z - 1, c)

    for j in range(per_device):
        units = pl.ds(j * unit, unit)
        remote(w_gate.at[units], gate_w.at[1, units], w_out.at[0, j], w_in.at[0, j], x_side)
        remote(w_up.at[units], up_w.at[1, units], w_out.at[1, j], w_in.at[1, j], x_side)
    @pl.when(above)
    def _():
        pass_on(z, me, z_up, tokens)

    @pl.when(below)
    def _():
        pass_on(zs + z, me, z_down, tokens)

    pass_on(2 * zs + z, me, y_side, tokens)
    pass_on(3 * zs + me // 2, me, mate, tokens)
    for j in range(chunks):
        remote(
            w_down.at[:, j * cd : (j + 1) * cd], down_far.at[j], d_out.at[j], d_in.at[j], x_side
        )
    for copy in own:
        copy.wait()

    def column(index, j):
        row = table[index, pl.ds(ex * per_device + j, 1), :]
        return jnp.transpose(jnp.broadcast_to(row, (rows, rows)))

    def scales(index):
        columns = [column(index, j) for j in range(per_device)]
        lanes = columns[0].shape[1]
        place = lax.broadcasted_iota(jnp.int32, (rows, lanes), 1)
        pieces = []
        for t in range(ff // lanes):
            piece = columns[0]
            for j in range(1, per_device):
                piece = jnp.where(place + t * lanes >= j * unit, columns[j], piece)
            pieces.append(piece)
        return jnp.concatenate(pieces, axis=1)

    nt = (((1,), (1,)), ((), ()))

    def act(block, gate_t, up_t):
        gate = lax.dot_general(block, gate_t, nt, preferred_element_type=jnp.float32)
        up = lax.dot_general(block, up_t, nt, preferred_element_type=jnp.float32)
        return gate / (1.0 + jnp.exp(-gate)) * up

    batch = 4

    def relay(source, onward, device, n):
        index = slot(y, source, c)
        arrived(index)

        @pl.when(onward)
        def _():
            pass_on(n + source, index, device)

        pass_on(2 * zs + source, index, y_side)
        pass_on(3 * zs + index // 2, index, mate)

    for d in range(1, zs):

        @pl.when(z >= d)
        def _():
            relay(z - d, above, z_up, 0)

        @pl.when(z + d < zs)
        def _():
            relay(z + d, below, z_down, zs)

    def from_y(source):
        index = slot(1 - y, source, c)
        arrived(index)
        pass_on(3 * zs + index // 2, index, mate)

    from_y(z)
    for d in range(1, zs):

        @pl.when(z >= d)
        def _():
            from_y(z - d)

        @pl.when(z + d < zs)
        def _():
            from_y(z + d)

    def from_mate(i, carry):
        arrived(2 * i + 1 - c)
        return carry

    lax.fori_loop(0, slots // 2, from_mate, 0)

    def own_half(q, carry):
        first = q * batch
        block = tok[pl.ds(first, batch)].reshape(batch * rows, width)
        value = act(block, gate_w[0], up_w[0])
        for i in range(batch):
            scaled = value[i * rows : (i + 1) * rows] * scales(first + i)
            hidden[first + i, :, 0:ff] = scaled.astype(jnp.bfloat16)
        return carry

    lax.fori_loop(0, slots // batch, own_half, 0)

    def add_tally(i, total):
        return total + table[i, experts : 2 * experts, :]

    tally[...] = lax.fori_loop(0, slots, add_tally, jnp.zeros((experts, rows), jnp.float32))

    remote(tally, tally_in, t_out, t_in, x_side)

    for j in range(per_device):
        units = pl.ds(j * unit, unit)
        landed(gate_w.at[1, units], w_in.at[0, j])
        landed(up_w.at[1, units], w_in.at[1, j])

        def other_half(q, carry, j=j):
            first = q * batch
            block = tok[pl.ds(first, batch)].reshape(batch * rows, width)
            value = act(block, gate_w[1, j * unit : (j + 1) * unit], up_w[1, j * unit : (j + 1) * unit])
            for i in range(batch):
                scaled = value[i * rows : (i + 1) * rows] * column(first + i, j)[:, 0:1]
                hidden[first + i, :, ff + j * unit : ff + (j + 1) * unit] = scaled.astype(
                    jnp.bfloat16
                )
            return carry

        if j < per_device - 1:
            lax.fori_loop(0, slots // batch, other_half, 0)

    groups = slots // batch // 2
    starts = ((1 - y) * groups, y * groups)

    def down(j, part):
        def step(q, carry):
            near = hidden[pl.ds(q * batch, batch)].reshape(batch * rows, 2 * ff)
            value = jnp.dot(
                near[:, :ff], down_own[:, j * cd : (j + 1) * cd],
                preferred_element_type=jnp.float32,
            ) + jnp.dot(near[:, ff:], down_far[j], preferred_element_type=jnp.float32)
            for i in range(batch // 2):
                one = value[2 * i * rows : (2 * i + 1) * rows]
                two = value[(2 * i + 1) * rows : (2 * i + 2) * rows]
                keep1[j, q * (batch // 2) + i] = jnp.where(c == 0, one, two)
                part1[j, q * (batch // 2) + i] = jnp.where(c == 0, two, one).astype(jnp.bfloat16)
            return carry

        lax.fori_loop(starts[part], starts[part] + groups, step, 0)
        held = pl.ds(starts[part] * (batch // 2), zs)
        remote(
            part1.at[j, held], recv1.at[j, held], s1_out.at[j, part], s1_in.at[j, part], mate
        )

    def over_core(j):
        landed(recv1.at[j, pl.ds((1 - y) * zs, zs)], s1_in.at[j, 0])

        def away(i, carry):
            n = (1 - y) * zs + i
            value = keep1[j, n] + recv1[j, n].astype(jnp.float32)
            part2[j, i] = value.astype(jnp.bfloat16)
            return carry

        lax.fori_loop(0, zs, away, 0)
        remote(part2.at[j], recv2.at[j], s2_out.at[j], s2_in.at[j], y_side)

        landed(recv1.at[j, pl.ds(y * zs, zs)], s1_in.at[j, 1])

        def home(i, carry):
            n = y * zs + i
            keep2[j, i] = keep1[j, n] + recv1[j, n].astype(jnp.float32)
            return carry

        lax.fori_loop(0, zs, home, 0)

    def over_y(j):
        landed(recv2.at[j], s2_in.at[j])

        for s in range(1, zs):
            n = far(s)
            value = keep2[j, n] + recv2[j, n].astype(jnp.float32)
            part3[j, s - 1] = value.astype(jnp.bfloat16)
            remote(
                part3.at[j, s - 1], recv3.at[j, s - 1],
                s3_out.at[j, s - 1], s3_in.at[j, s - 1], at(y, x, n, c),
            )
        keep3[j] = keep2[j, z] + recv2[j, z].astype(jnp.float32)

    def over_z(j):
        value = keep3[j]
        for s in range(1, zs):
            landed(recv3.at[j, s - 1], s3_in.at[j, s - 1])
            value += recv3[j, s - 1].astype(jnp.float32)
        out[:, j * cd : (j + 1) * cd] = value.astype(jnp.bfloat16)

    for j in range(chunks + 3):
        if j < chunks:
            if j > 0:
                landed(down_far.at[j], d_in.at[j])
            for part in range(2):
                if j == 0:
                    lax.fori_loop(starts[part], starts[part] + groups, other_half, 0)
                    if part == 0:
                        landed(down_far.at[0], d_in.at[0])
                down(j, part)
        if 0 <= j - 1 < chunks:
            over_core(j - 1)
        if 0 <= j - 2 < chunks:
            over_y(j - 2)
        if 0 <= j - 3 < chunks:
            over_z(j - 3)

    landed(tally_in, t_in)
    count = jnp.sum(tally[...] + tally_in[...], axis=1, keepdims=True)
    totals[...] = jnp.broadcast_to(count, totals.shape)
    for copy in sent:
        copy.wait_send()

    def z_sent(source, carry):
        @pl.when(jnp.logical_and(above, source <= z))
        def _():
            passed(source)

        @pl.when(jnp.logical_and(below, source >= z))
        def _():
            passed(zs + source)

        passed(2 * zs + source)
        return carry

    lax.fori_loop(0, zs, z_sent, 0)

    def mate_sent(i, carry):
        passed(3 * zs + i)
        return carry

    lax.fori_loop(0, slots // 2, mate_sent, 0)


def group_scratch(zs, rows, width, ff, experts):
    slots = 4 * zs
    cd = width // chunks
    bf, f32 = jnp.bfloat16, jnp.float32
    return [
        ((slots, rows, width), bf),
        ((slots, 2 * experts, rows), f32),
        ((2, ff, width), bf),
        ((2, ff, width), bf),
        ((ff, width), bf),
        ((chunks, ff, cd), bf),
        ((slots, rows, 2 * ff), bf),
        ((chunks, slots // 2, rows, cd), bf),
        ((chunks, slots // 2, rows, cd), f32),
        ((chunks, slots // 2, rows, cd), bf),
        ((chunks, zs, rows, cd), bf),
        ((chunks, zs, rows, cd), f32),
        ((chunks, zs, rows, cd), bf),
        ((chunks, zs - 1, rows, cd), bf),
        ((chunks, rows, cd), f32),
        ((chunks, zs - 1, rows, cd), bf),
        ((experts, rows), f32),
        ((experts, rows), f32),
    ]


def group_body(zs, tokens, routes, route_weight, bias, w_gate, w_up, w_down):
    rows, width = tokens.shape
    experts = bias.shape[0]
    per_device, unit, _ = w_gate.shape
    ff = per_device * unit
    top = routes.shape[1]
    capacity = 5 * rows * top // (4 * experts)
    slots = 4 * zs
    dma = pltpu.SemaphoreType.DMA
    vmem = pl.BlockSpec(memory_space=pltpu.VMEM)
    anywhere = pl.BlockSpec(memory_space=pl.ANY)
    mixed, totals = pl.pallas_call(
        functools.partial(layer_kernel, zs, capacity, per_device),
        out_shape=(
            jax.ShapeDtypeStruct((rows, width), jnp.bfloat16),
            jax.ShapeDtypeStruct((experts, rows), jnp.float32),
        ),
        in_specs=[anywhere, vmem, vmem, anywhere, anywhere, anywhere],
        out_specs=(vmem, vmem),
        scratch_shapes=[
            pltpu.VMEM(shape, kind)
            for shape, kind in group_scratch(zs, rows, width, ff, experts)
        ]
        + [
            dma((slots,)), dma((5 * zs,)), dma((slots,)), dma((5 * zs,)), dma((4,)),
            dma((2, per_device)), dma((2, per_device)), dma((chunks,)), dma((chunks,)),
            dma((chunks, 2)), dma((chunks, 2)), dma((chunks,)), dma((chunks,)),
            dma((chunks, zs - 1)), dma((chunks, zs - 1)), dma, dma,
        ],
        compiler_params=pltpu.CompilerParams(
            collective_id=0, has_side_effects=True, vmem_limit_bytes=VMEM_BYTES
        ),
    )(
        tokens, routes.T, route_weight.T,
        w_gate.reshape(ff, width), w_up.reshape(ff, width), w_down.reshape(ff, width),
    )
    counts = totals[:, 0]
    mean_load = rows * top * lax.axis_size("dp") * lax.axis_size("expert")
    new_bias = bias + bias_rate * jnp.sign(mean_load - experts * counts)
    return (mixed, new_bias, counts.astype(jnp.int32))


def body(tokens, routes, route_weight, bias, w_gate, w_up, w_down):
    rows, width = tokens.shape
    per_device, unit, _ = w_gate.shape
    groups = lax.axis_size("expert")
    zs = groups // 2
    held = group_scratch(zs, rows, width, per_device * unit, bias.shape[0])
    total = 0
    for shape, kind in held:
        size = jnp.dtype(kind).itemsize
        for extent in shape:
            size *= extent
        total += size
    args = (tokens, routes, route_weight, bias, w_gate, w_up, w_down)
    if lax.axis_size("dp") == 4 and groups % 2 == 0 and zs % 2 == 0 and total < 0.85 * VMEM_BYTES:
        return group_body(zs, *args)
    return exchange_body(*args)


def solution(mesh):
    placed = (
        P(("dp", "expert"), None),
        P(("dp", "expert"), None),
        P(("dp", "expert"), None),
        P(),
        P("expert", "dp", None),
        P("expert", "dp", None),
        P("expert", "dp", None),
    )
    return jax.shard_map(
        body,
        mesh=mesh,
        in_specs=placed,
        out_specs=(P(("dp", "expert"), None), P(), P()),
        check_vma=False,
    )
```
